32 devices in a mesh: zero: 2 (over x), cols: 16 (over z, y, core).
Axes of the slice: x: 2, y: 2, z: 4, core: 2. Of those that a mesh axis runs over, the one named last changes fastest.
Arguments:
- train_gate: bfloat16 [5120, 25600], P('zero', 'cols'), may hold values from -0.125 to 0.125
- low_gate: bfloat16 [5120, 64], P('zero'), may hold values from -0.078125 to 0.078125
- high_gate: bfloat16 [64, 25600], P(None, 'cols'), may hold values from -0.75 to 0.75
- train_up: bfloat16 [5120, 25600], P('zero', 'cols'), may hold values from -0.125 to 0.125
- low_up: bfloat16 [5120, 64], P('zero'), may hold values from -0.078125 to 0.078125
- high_up: bfloat16 [64, 25600], P(None, 'cols'), may hold values from -0.75 to 0.75
- norm_train: float32 [5120], P(('zero', 'cols')), may hold values from 0.25 to 1.75
- norm_step: float32 [5120], P(('zero', 'cols')), may hold values from -0.3 to 0.3
Outputs:
- ready_gate: bfloat16 [5120, 25600], P(None, 'cols')
- ready_up: bfloat16 [5120, 25600], P(None, 'cols')
- column_gate: float32 [25600], P('cols')
- column_up: float32 [25600], P('cols')
- serve_norm: bfloat16 [5120], replicated
The draws below stay inside these ranges and needn't reach their ends.
All inputs are finite; a program needn't handle non-finite values.
Results may differ from the reference program's by a relative error of at most 0.001.
Values may be sent and summed in bfloat16 or wider, within the bound.
A program may use at most 128 MiB of HBM per device.

```python
import jax
import jax.numpy as jnp
from jax import lax

D_MODEL = 5120
D_INNER = 25600
RANK = 64


def raised(entries, key, source, target, shards_of, factor):
    def block_of(dim):
        return (jnp.arange(entries.shape[dim]) // (entries.shape[dim] // shards_of)).reshape((-1,) + (1,) * (entries.ndim - 1 - dim))

    one_side = jax.random.permutation(key, shards_of)[block_of(target)]
    other_side = (block_of(target) + shards_of // 2) % shards_of
    return jnp.where((block_of(source) == one_side) | (block_of(source) == other_side), factor * entries, entries)


def levels(own_key, dims, split, smallest, high):
    def one(dim, parts):
        heights = jax.random.uniform(jax.random.fold_in(jax.random.fold_in(own_key, 6), dim), (parts,), jnp.float32, smallest / len(split), high / len(split))
        return jnp.repeat(jnp.exp(heights), dims[dim] // parts).reshape((-1,) + (1,) * (len(dims) - dim - 1))

    loudness = one(*split[0])
    for cut in split[1:]:
        loudness = loudness * one(*cut)
    return loudness


def normal_values(key, dims, deviation, reach, shards=(), dtype=jnp.bfloat16):
    entries = jax.random.normal(key, dims, jnp.float32) * deviation
    if len(shards) > 0:
        entries = levels(key, dims, shards, -0.22, 0.18) * entries
    return jnp.clip(entries, min=-reach, max=reach).astype(dtype)


def bell_draw_with(key, extent, width, limit, pieces, heavy, kind=jnp.bfloat16):
    drawn = width * jax.random.normal(key, extent, jnp.float32)
    if pieces:
        drawn = drawn * levels(key, extent, pieces, -0.22, 0.18)
    return jnp.clip(raised(drawn, jax.random.fold_in(key, 3), *heavy), -limit, limit).astype(kind)


def setup_inputs(seed: int = 0) -> dict:
    seeds = jax.random.split(jax.random.key(seed), 9)
    return {
        "train_gate": bell_draw_with(seeds[0], (D_MODEL, D_INNER), D_MODEL ** -0.5, 0.125, ((0, 2), (1, 16)), (0, 1, 16, 2.0)),
        "low_gate": normal_values(seeds[1], (D_MODEL, RANK), D_MODEL ** -0.5, 0.078125, ((0, 2),)),
        "high_gate": normal_values(seeds[2], (RANK, D_INNER), RANK ** -0.5, 0.75, ((1, 16),)),
        "train_up": bell_draw_with(seeds[3], (D_MODEL, D_INNER), D_MODEL ** -0.5, 0.125, ((0, 2), (1, 16)), (0, 1, 16, 2.0)),
        "low_up": normal_values(seeds[4], (D_MODEL, RANK), D_MODEL ** -0.5, 0.078125, ((0, 2),)),
        "high_up": normal_values(seeds[5], (RANK, D_INNER), RANK ** -0.5, 0.75, ((1, 16),)),
        "norm_train": jnp.clip(1.0 + 0.15 * jax.random.normal(seeds[6], (D_MODEL,), jnp.float32), 0.25, 1.75),
        "norm_step": jnp.clip(jax.random.uniform(seeds[7], (D_MODEL,), jnp.float32, -0.3, 0.3) * levels(seeds[7], (D_MODEL,), ((0, 32),), -0.4, 0.0), -0.3, 0.3),
    }


mix_rate = 2.0

def reference(train_gate, low_gate, high_gate, train_up, low_up, high_up, norm_train, norm_step):
    latest_gate = train_gate.astype(jnp.float32) + mix_rate * jnp.dot(low_gate, high_gate, preferred_element_type=jnp.float32)
    latest_up = train_up.astype(jnp.float32) + mix_rate * jnp.dot(low_up, high_up, preferred_element_type=jnp.float32)
    column_gate = jnp.sqrt(lax.optimization_barrier(jnp.sum(latest_gate * latest_gate, axis=0)))
    ready_gate = (latest_gate / column_gate).astype(jnp.bfloat16)
    column_up = jnp.sqrt(lax.optimization_barrier(jnp.sum(latest_up * latest_up, axis=0)))
    ready_up = (latest_up / column_up).astype(jnp.bfloat16)
    serve_norm = (norm_train + norm_step).astype(jnp.bfloat16)
    return (ready_gate, ready_up, column_gate, column_up, serve_norm)
```

```python
import functools

import jax
import jax.numpy as jnp
from jax import lax
from jax.experimental import pallas as pl
from jax.experimental.pallas import tpu as pltpu
from jax.sharding import PartitionSpec as P

mix_rate = 2.0


def merge_kernel(n, rows, extra, *refs):
    parts, (high_ref, low_ref) = refs[:n], refs[n:n + 2]
    out_ref, column_ref, latest_ref = refs[n + 2 + extra:]
    me = lax.axis_index("zero")
    high = high_ref[...] * mix_rate
    total = None
    for shift in range(n):
        span = pl.ds(shift * rows, rows)
        latest = parts[shift][...].astype(jnp.float32) + lax.dot_general(
            high, low_ref[:, span], (((1,), (0,)), ((), ())), preferred_element_type=jnp.float32
        )
        latest_ref[:, span] = latest
        squares = jnp.sum(latest * latest, axis=1, keepdims=True)
        total = squares if total is None else total + squares
    column = jnp.sqrt(total)
    column_ref[...] = column
    inverse = 1.0 / column
    for shift in range(n):
        owner = lax.rem(me + shift, n)
        there = pl.ds(pl.multiple_of(owner * rows, 128), rows)
        out_ref[:, there] = (latest_ref[:, pl.ds(shift * rows, rows)] * inverse).astype(jnp.bfloat16)


def merge(own, received, high, low, ready, after, first, block):
    n = len(received) + 1
    width, rows = received[0].shape
    rank = high.shape[1]
    shift = first // block
    aliased = 0 if ready is None else 1
    here = lambda i: (i + shift, 0)
    plain = lambda i: (i, 0)
    in_specs = [pl.BlockSpec((block, rows), here)]
    in_specs += [pl.BlockSpec((block, rows), plain)] * (n - 1)
    in_specs += [pl.BlockSpec((block, rank), here), pl.BlockSpec((rank, n * rows), lambda i: (0, 0))]
    operands = [own, *received, high, low]
    if aliased:
        in_specs.append(pl.BlockSpec(memory_space=pl.ANY))
        operands.append(ready)
    if after is not None:
        in_specs.append(pl.BlockSpec(memory_space=pl.ANY))
        operands.append(after)
    moved = 2 * width * n * rows * 2
    return pl.pallas_call(
        functools.partial(merge_kernel, n, rows, len(operands) - n - 2),
        grid=(width // block,),
        out_shape=(
            jax.ShapeDtypeStruct((own.shape[0], n * rows), jnp.bfloat16),
            jax.ShapeDtypeStruct((width, 1), jnp.float32),
        ),
        in_specs=in_specs,
        out_specs=(pl.BlockSpec((block, n * rows), here), pl.BlockSpec((block, 1), plain)),
        scratch_shapes=[pltpu.VMEM((block, n * rows), jnp.float32)],
        input_output_aliases={n + 2: 0} if aliased else {},
        cost_estimate=pl.CostEstimate(flops=2 * width * n * rows * rank, bytes_accessed=moved, transcendentals=0),
    )(*operands)


def pieces_of(total, fractions):
    sizes, left = [], total
    for fraction in fractions:
        take = min(left, max(1, int(total * fraction)))
        if take > 0:
            sizes.append(take)
        left -= take
    if left > 0:
        sizes[0] += left
    return sizes


def on_device(n, train_gate, low_gate, high_gate, train_up, low_up, high_up, norm_train, norm_step):
    rings = [[((k + shift) % n, k) for k in range(n)] for shift in range(1, n)]

    def from_others(values):
        return [lax.ppermute(values, "zero", ring) for ring in rings]

    rank = low_gate.shape[1]
    n_cols = lax.axis_size("cols")
    lows = jnp.concatenate([low_gate.T, low_up.T], axis=0)
    share = 2 * rank // n_cols
    mine = lax.dynamic_slice_in_dim(lows, lax.axis_index("cols") * share, share, axis=0)
    others_low = [lax.all_gather(p, "cols", axis=0, tiled=True) for p in from_others(mine)]
    every_low = jnp.concatenate([lows, *others_low], axis=1)
    gain = (norm_train + norm_step).astype(jnp.bfloat16)
    gains = jnp.stack([gain, *from_others(gain)])
    gains = lax.all_gather(gains, "cols", axis=1, tiled=True)
    me = lax.axis_index("zero")
    serve_norm = jnp.concatenate([gains[(k - me) % n] for k in range(n)])

    gate, up = train_gate.T, train_up.T
    width = gate.shape[0]
    block = next(b for b in (64, 32, 16, 8) if width % b == 0)
    got_gate = from_others(gate)
    got_up, first = [], 0
    for size in pieces_of(width // block, (0.68, 0.24, 0.08)):
        got_up.append((first, from_others(lax.slice_in_dim(up, first, first + size * block, axis=0))))
        first += size * block

    ready_gate, column_gate = merge(gate, got_gate, high_gate.T, every_low[:rank], None, None, 0, block)
    ready_up, columns = None, []
    for first, received in got_up:
        ready_up, column = merge(up, received, high_up.T, every_low[rank:], ready_up, None if columns else column_gate, first, block)
        columns.append(column)
    return (
        ready_gate.T,
        ready_up.T,
        column_gate.reshape(width),
        jnp.concatenate(columns, axis=0).reshape(width),
        serve_norm,
    )


def solution(mesh):
    return jax.shard_map(
        functools.partial(on_device, mesh.shape["zero"]),
        mesh=mesh,
        in_specs=(
            P("zero", "cols"),
            P("zero", None),
            P(None, "cols"),
            P("zero", "cols"),
            P("zero", None),
            P(None, "cols"),
            P(("zero", "cols")),
            P(("zero", "cols")),
        ),
        out_specs=(P(None, "cols"), P(None, "cols"), P("cols"), P("cols"), P()),
        check_vma=False,
    )
```

```python
import functools

import jax
import jax.numpy as jnp
from jax import lax
from jax.experimental import pallas as pl
from jax.experimental.pallas import tpu as pltpu
from jax.sharding import PartitionSpec as P


mix_rate = 2.0


def merge_kernel(n, rows, extra, *refs):
    parts, (high_ref, low_ref) = refs[:n], refs[n:n + 2]
    out_ref, column_ref, latest_ref = refs[n + 2 + extra:]
    me = lax.axis_index("zero")
    high = high_ref[...] * mix_rate
    total = None
    for shift in range(n):
        span = pl.ds(shift * rows, rows)
        latest = parts[shift][...].astype(jnp.float32) + lax.dot_general(
            high, low_ref[:, span], (((1,), (0,)), ((), ())), preferred_element_type=jnp.float32
        )
        latest_ref[:, span] = latest
        squares = jnp.sum(latest * latest, axis=1, keepdims=True)
        total = squares if total is None else total + squares
    column = jnp.sqrt(total)
    column_ref[...] = column
    inverse = 1.0 / column
    for shift in range(n):
        owner = lax.rem(me + shift, n)
        there = pl.ds(pl.multiple_of(owner * rows, 128), rows)
        out_ref[:, there] = (latest_ref[:, pl.ds(shift * rows, rows)] * inverse).astype(jnp.bfloat16)


def merge(own, received, high, low, ready, after, first, block):
    n = len(received) + 1
    width, rows = received[0].shape
    rank = high.shape[1]
    shift = first // block
    aliased = 0 if ready is None else 1
    here = lambda i: (i + shift, 0)
    plain = lambda i: (i, 0)
    in_specs = [pl.BlockSpec((block, rows), here)]
    in_specs += [pl.BlockSpec((block, rows), plain)] * (n - 1)
    in_specs += [pl.BlockSpec((block, rank), here), pl.BlockSpec((rank, n * rows), lambda i: (0, 0))]
    operands = [own, *received, high, low]
    if aliased:
        in_specs.append(pl.BlockSpec(memory_space=pl.ANY))
        operands.append(ready)
    if after is not None:
        in_specs.append(pl.BlockSpec(memory_space=pl.ANY))
        operands.append(after)
    moved = 2 * width * n * rows * 2
    return pl.pallas_call(
        functools.partial(merge_kernel, n, rows, len(operands) - n - 2),
        grid=(width // block,),
        out_shape=(
            jax.ShapeDtypeStruct((own.shape[0], n * rows), jnp.bfloat16),
            jax.ShapeDtypeStruct((width, 1), jnp.float32),
        ),
        in_specs=in_specs,
        out_specs=(pl.BlockSpec((block, n * rows), here), pl.BlockSpec((block, 1), plain)),
        scratch_shapes=[pltpu.VMEM((block, n * rows), jnp.float32)],
        input_output_aliases={n + 2: 0} if aliased else {},
        cost_estimate=pl.CostEstimate(flops=2 * width * n * rows * rank, bytes_accessed=moved, transcendentals=0),
    )(*operands)


def last_kernel(n, rows, first, *refs):
    received, (own_ref, delta_ref, part_ref) = refs[:n - 1], refs[n - 1:n + 2]
    out_ref, column_ref, made_ref, sem = refs[n + 4:]
    me = lax.axis_index("zero")
    width = own_ref.shape[0]
    latests, total = [own_ref[...]], part_ref[...]
    for shift in range(1, n):
        span = pl.ds((shift - 1) * rows, rows)
        latest = received[shift - 1][...].astype(jnp.float32) + delta_ref[:, span]
        total = total + jnp.sum(latest * latest, axis=1, keepdims=True)
        latests.append(latest)
    column = jnp.sqrt(total)
    inverse = 1.0 / column
    for shift in range(n):
        there = pl.ds(pl.multiple_of(lax.rem(me + shift, n) * rows, 128), rows)
        made_ref[:, there] = (latests[shift] * inverse).astype(jnp.bfloat16)
    copy = pltpu.make_async_copy(made_ref, out_ref.at[pl.ds(first, width), :], sem)
    copy.start()
    eye = lax.broadcasted_iota(jnp.int32, (width, width), 0) == lax.broadcasted_iota(jnp.int32, (width, width), 1)
    column_ref[...] = jnp.sum(jnp.where(eye, column, 0.0), axis=0, keepdims=True)
    copy.wait()


def merge_last(received, own, delta, part, ready, after, first):
    n = len(received) + 1
    width, rows = own.shape
    vmem, anywhere = pl.BlockSpec(memory_space=pltpu.VMEM), pl.BlockSpec(memory_space=pl.ANY)
    return pl.pallas_call(
        functools.partial(last_kernel, n, rows, first),
        out_shape=(
            jax.ShapeDtypeStruct(ready.shape, jnp.bfloat16),
            jax.ShapeDtypeStruct((1, width), jnp.float32),
        ),
        in_specs=[vmem] * (n + 2) + [anywhere] * 2,
        out_specs=(anywhere, vmem),
        scratch_shapes=[pltpu.VMEM((width, n * rows), jnp.bfloat16), pltpu.SemaphoreType.DMA],
        input_output_aliases={n + 2: 0},
        cost_estimate=pl.CostEstimate(flops=8 * width * n * rows, bytes_accessed=8 * width * n * rows, transcendentals=0),
    )(*received, own, delta, part, ready, after)


def pieces_of(total):
    small = [max(1, int(total * fraction)) for fraction in (0.08, 0.16, 0.06, 0.02)]
    return [small[0], total - sum(small), *small[1:]]


def block_of(*spans):
    return next(b for b in (64, 32, 16, 8) if all(s % b == 0 for s in spans))


def on_device(n, train_gate, low_gate, high_gate, train_up, low_up, high_up, norm_train, norm_step):
    rings = [[((k + shift) % n, k) for k in range(n)] for shift in range(1, n)]

    def from_others(values):
        return [lax.ppermute(values, "zero", ring) for ring in rings]

    gate, up = train_gate.T, train_up.T
    width, rows = gate.shape
    unit = block_of(width)
    unit = min(unit, 32)
    pieces, first = [], 0
    for size in pieces_of(width // unit):
        pieces.append((first, lax.slice_in_dim(up, first, first + size * unit, axis=0)))
        first += size * unit

    got_up = [from_others(pieces[0][1])]
    rank = low_gate.shape[1]
    share = 2 * rank // lax.axis_size("cols")
    lows = jnp.concatenate([low_gate.T, low_up.T], axis=0)
    mine = lax.dynamic_slice_in_dim(lows, lax.axis_index("cols") * share, share, axis=0)
    got_low = from_others(mine)
    gain = (norm_train + norm_step).astype(jnp.bfloat16)
    got_gain = from_others(gain)
    got_gate = from_others(gate)
    for first, piece in pieces[1:]:
        got_up.append(from_others(piece))

    others_low = [lax.all_gather(p, "cols", axis=0, tiled=True) for p in got_low]
    every_low = jnp.concatenate([lows, *others_low], axis=1)
    low_for_gate, low_for_up = every_low[:rank], every_low[rank:]
    gains = lax.all_gather(jnp.stack([gain, *got_gain]), "cols", axis=1, tiled=True)
    me = lax.axis_index("zero")
    serve_norm = jnp.concatenate([gains[(k - me) % n] for k in range(n)])

    high_for_up = high_up.T
    first, own = pieces[-1]
    delta = mix_rate * jnp.dot(high_for_up[first:], low_for_up, preferred_element_type=jnp.float32)
    latest = own.astype(jnp.float32) + delta[:, :rows]
    part = jnp.sum(latest * latest, axis=1, keepdims=True)
    delta = delta[:, rows:]

    ready_up, column = merge(up, got_up[0], high_for_up, low_for_up, None, None, 0, block_of(pieces[0][1].shape[0]))
    columns = [column]
    ready_gate, column_gate = merge(gate, got_gate, high_gate.T, low_for_gate, None, column, 0, block_of(width))
    after = column_gate
    for (first, piece), received in zip(pieces[1:-1], got_up[1:-1]):
        block = block_of(first, piece.shape[0])
        ready_up, column = merge(up, received, high_for_up, low_for_up, ready_up, after, first, block)
        columns.append(column)
        after = part
    ready_up, last = merge_last(got_up[-1], latest, delta, part, ready_up, column, pieces[-1][0])
    columns = [column.reshape(-1) for column in columns] + [last.reshape(-1)]
    return (ready_gate.T, ready_up.T, column_gate.reshape(width), jnp.concatenate(columns), serve_norm)


def in_layer(n, *arrays):
    return on_device(n, *arrays)


def solution(mesh):
    return jax.shard_map(
        functools.partial(in_layer, mesh.shape["zero"]),
        mesh=mesh,
        in_specs=(
            P("zero", "cols"),
            P("zero", None),
            P(None, "cols"),
            P("zero", "cols"),
            P("zero", None),
            P(None, "cols"),
            P(("zero", "cols")),
            P(("zero", "cols")),
        ),
        out_specs=(P(None, "cols"), P(None, "cols"), P("cols"), P("cols"), P()),
        check_vma=False,
    )
```
